8 devices in a mesh: prob: 2 (over z, y), feat: 4 (over x, core).
Axes of the slice: x: 2, y: 2, z: 1, core: 2. Of those that a mesh axis runs over, the one named last changes fastest.
Arguments:
- x_data: bfloat16 [4096, 784], P('prob'), parts along dimension 0
- targets: float32 [4096], P('prob'), parts along dimension 0
- w_in: float32 [2048, 784], P(('prob', 'feat')), parts along dimension 0
- w_out: float32 [2048], P(('prob', 'feat')), parts along dimension 0
- reg_weight: float32 [2], P('prob'), parts along dimension 0
- step_size: float32 [2], P('prob'), parts along dimension 0
Outputs:
- output 1: float32 [2048, 784], P(('prob', 'feat')), parts along dimension 0
- output 2: float32 [2048], P(('prob', 'feat')), parts along dimension 0
- output 3: float32 [12], P('prob'), parts along dimension 0
There are 2 independent parts. The reference program is written for one: setup_inputs(seed, part) draws one part's arguments, and reference() takes and returns one part's arrays. A program takes and returns all parts, laid end to end along the dimension named above; each array names one.
All inputs are finite; a program needn't handle non-finite values.
Results may differ from the reference program's by a relative error of at most 0.001.
Values are sent between devices in bfloat16 or wider.
A program may use at most 1 GiB of HBM per device.

```python
import math
import jax
import jax.numpy as jnp
from jax import lax

NUM_ROWS = 2048
IN_DIM = 784
HIDDEN = 1024
NUM_ITERS = 6
HIST_LEN = 3

IN_SCALE = 1.0 / math.sqrt(IN_DIM)
OUT_SCALE = 1.0 / math.sqrt(HIDDEN)


def setup_inputs(seed: int = 0, part: int = 0) -> dict:
    base_key = jax.random.fold_in(jax.random.key(seed), part)
    sub_keys = jax.random.split(base_key, 7)
    labels = jax.random.randint(sub_keys[0], (NUM_ROWS,), 0, 2)
    label_sign = (2 * labels - 1).astype(jnp.float32)
    mean_dir = 0.5 * jax.random.normal(sub_keys[1], (IN_DIM,), jnp.float32)
    noise_mat = jax.random.normal(sub_keys[2], (NUM_ROWS, IN_DIM), jnp.float32)
    x_data = (noise_mat + label_sign[:, None] * mean_dir[None, :]).astype(jnp.bfloat16)
    unit_pos = jnp.arange(HIDDEN, dtype=jnp.float32) / HIDDEN
    row_scale = jnp.exp2(2.0 * unit_pos - 1.0)
    w_in = jax.random.normal(sub_keys[3], (HIDDEN, IN_DIM), jnp.float32) * row_scale[:, None]
    w_out = jax.random.normal(sub_keys[4], (HIDDEN,), jnp.float32)
    reg_weight = jax.random.uniform(sub_keys[5], (1,), jnp.float32, 0.01, 0.02)
    step_size = jax.random.uniform(sub_keys[6], (1,), jnp.float32, 0.08, 0.2)
    return {"x_data": x_data, "targets": labels.astype(jnp.float32), "w_in": w_in, "w_out": w_out, "reg_weight": reg_weight, "step_size": step_size}


def fit_loss(w_in, w_out, x_f32, targets):
    pre_act = lax.dot_general(x_f32, w_in, (((1,), (1,)), ((), ()))) * IN_SCALE
    logits = jnp.dot(jnp.tanh(pre_act), w_out) * OUT_SCALE
    return jnp.mean(jax.nn.softplus(logits) - targets * logits)


def pair_dot(first, second):
    return jnp.sum(first[0] * second[0]) + jnp.sum(first[1] * second[1])


def pair_axpy(base, coef, other):
    return (base[0] + coef * other[0], base[1] + coef * other[1])


def two_loop(full_grad, hist_s, hist_y, rho_vals, gamma_scale, dot_fn):
    query_vec = full_grad
    a_coefs = {}
    for pos_idx in reversed(range(len(hist_s))):
        a_coefs[pos_idx] = rho_vals[pos_idx] * dot_fn(hist_s[pos_idx], query_vec)
        query_vec = pair_axpy(query_vec, -a_coefs[pos_idx], hist_y[pos_idx])
    result = (gamma_scale * query_vec[0], gamma_scale * query_vec[1])
    for pos_idx in range(len(hist_s)):
        b_coef = rho_vals[pos_idx] * dot_fn(hist_y[pos_idx], result)
        result = pair_axpy(result, a_coefs[pos_idx] - b_coef, hist_s[pos_idx])
    return result


def reference(x_data, targets, w_in, w_out, reg_weight, step_size):
    x_f32 = x_data.astype(jnp.float32)
    reg_coef = reg_weight[0]
    step_coef = step_size[0]
    loss_grad = jax.value_and_grad(fit_loss, argnums=(0, 1))
    params = (w_in, w_out)
    prev_params = params
    prev_grad = params
    hist_s = []
    hist_y = []
    rho_vals = []
    losses = []
    for iter_idx in range(NUM_ITERS):
        loss_val, fit_grad = loss_grad(params[0], params[1], x_f32, targets)
        losses.append(loss_val)
        full_grad = pair_axpy(fit_grad, reg_coef, params)
        if iter_idx == 0:
            direction = full_grad
        else:
            s_vec = pair_axpy(params, -1.0, prev_params)
            y_vec = pair_axpy(full_grad, -1.0, prev_grad)
            curv_ys = pair_dot(y_vec, s_vec)
            hist_s = (hist_s + [s_vec])[-HIST_LEN:]
            hist_y = (hist_y + [y_vec])[-HIST_LEN:]
            rho_vals = (rho_vals + [1.0 / curv_ys])[-HIST_LEN:]
            gamma_scale = curv_ys / pair_dot(y_vec, y_vec)
            direction = two_loop(full_grad, hist_s, hist_y, rho_vals, gamma_scale, pair_dot)
        prev_params = params
        prev_grad = full_grad
        params = pair_axpy(params, -step_coef, direction)
    return params[0], params[1], jnp.stack(losses)
```

```python
import functools
import math

import jax
import jax.numpy as jnp
from jax import lax
from jax.experimental import pallas as pl
from jax.experimental.pallas import tpu as pltpu
from jax.sharding import PartitionSpec as P

NUM_ITERS = 6
HIST = 3
LANES = 128
CHUNK = 512
F32 = jnp.float32
BF16 = jnp.bfloat16
NT = (((1,), (1,)), ((), ()))
NN = (((1,), (0,)), ((), ()))


def split3(val):
    hi = val.astype(BF16)
    rest = val - hi.astype(F32)
    mid = rest.astype(BF16)
    lo = (rest - mid.astype(F32)).astype(BF16)
    return hi, mid, lo


def exact_dot(parts, rhs, dims):
    out = lax.dot_general(parts[0], rhs, dims, preferred_element_type=F32)
    for part in parts[1:]:
        out = out + lax.dot_general(part, rhs, dims, preferred_element_type=F32)
    return out


def sub_sum(val):
    return jnp.sum(val, axis=0, keepdims=True)


def kernel(feat, reg_ref, step_ref, x_ref, t_ref, w_ref, w2_ref, wout_ref, w2out_ref, loss_ref,
           theta, grad, hist_s, hist_y, p_hi, p_mid, p_lo, act, w2b, d_hi, d_mid, d_lo, zbuf, dbuf,
           z_send, z_recv, d_send, d_recv):
    rows, dim = x_ref.shape
    hid = w_ref.shape[0]
    wide = theta.shape[1]
    tail = dim // LANES * LANES
    tail_n = dim - tail
    n_chunks = rows // CHUNK
    q_n = CHUNK // LANES
    in_scale = 1.0 / math.sqrt(dim)
    out_scale = 1.0 / math.sqrt(hid * feat)
    me = lax.axis_index("feat")
    parts_refs = (p_hi, p_mid, p_lo)

    barrier = pltpu.get_barrier_semaphore()
    for off in range(1, feat):
        pl.semaphore_signal(barrier, inc=1, device_id={"feat": lax.rem(me + off, feat)}, device_id_type=pl.DeviceIdType.MESH)
    pl.semaphore_wait(barrier, feat - 1)

    def z_copy(c, off):
        return pltpu.make_async_remote_copy(
            src_ref=zbuf.at[me, c], dst_ref=zbuf.at[me, c], send_sem=z_send.at[c, off - 1], recv_sem=z_recv.at[c, off - 1],
            device_id={"feat": lax.rem(me + off, feat)}, device_id_type=pl.DeviceIdType.MESH)

    def d_copy(off):
        return pltpu.make_async_remote_copy(
            src_ref=dbuf.at[me], dst_ref=dbuf.at[me], send_sem=d_send.at[off - 1], recv_sem=d_recv.at[off - 1],
            device_id={"feat": lax.rem(me + off, feat)}, device_id_type=pl.DeviceIdType.MESH)

    lam = reg_ref[0]
    alpha = step_ref[0]
    lane = lax.broadcasted_iota(jnp.int32, (hid, LANES), 1)

    for j in range(hid // LANES):
        row = w2_ref[j:j + 1, :]
        w2b[j * LANES:(j + 1) * LANES, :] = jnp.transpose(jnp.broadcast_to(row, (LANES, LANES)))
    theta[:, :tail] = w_ref[:, :tail]
    w2_all = w2b[...]
    theta[:, tail:] = jnp.where(lane == tail_n, w2_all, 0.0)
    theta[:, tail:dim] = w_ref[:, tail:]
    for ref in (hist_s, hist_y):
        ref[...] = jnp.zeros_like(ref)
    grad[...] = jnp.zeros_like(grad)
    for g in range(hid // 16):
        sl = slice(16 * g, 16 * g + 16)
        for ref, val in zip(parts_refs, split3(theta[sl, :])):
            ref[sl, :] = val

    row1 = jnp.zeros((8, LANES), F32)

    def iteration(k, carry):
        rho0p, rho1p, sg0p, sg1p, yg0p, yg1p, yy00p, yy01p, yy11p, sy01p = carry
        n0 = lax.rem(k, HIST)
        n1 = lax.rem(k + 2, HIST)
        n2 = lax.rem(k + 1, HIST)
        live = k > 0

        for c in range(n_chunks):
            cols = slice(CHUNK * c, CHUNK * (c + 1))
            act[:, cols] = exact_dot([ref[:, :dim] for ref in parts_refs], x_ref[cols, :], NT)
            acc = jnp.zeros((8, CHUNK), F32)
            for g in range(hid // 8):
                sl = slice(8 * g, 8 * g + 8)
                h = jnp.tanh(act[sl, cols] * in_scale)
                act[sl, cols] = h
                acc = acc + h * jnp.concatenate([w2b[sl, :]] * q_n, axis=1)
            zrow = sub_sum(acc) * out_scale
            for q in range(q_n):
                zbuf[me, c, q:q + 1, :] = zrow[:, LANES * q:LANES * (q + 1)]
            for off in range(1, feat):
                z_copy(c, off).start()

        loss_acc = jnp.zeros((q_n, LANES), F32)
        gcol = [jnp.zeros((16, LANES), F32) for _ in range(hid // 16)]
        for c in range(n_chunks):
            cols = slice(CHUNK * c, CHUNK * (c + 1))
            for off in range(1, feat):
                z_copy(c, off).wait()
            z = zbuf[0, c]
            for src in range(1, feat):
                z = z + zbuf[src, c]
            t = t_ref[c]
            ez = jnp.exp(-jnp.abs(z))
            loss_acc = loss_acc + (jnp.maximum(z, 0.0) + jnp.log1p(ez) - t * z)
            sig = jnp.where(z >= 0.0, 1.0, ez) / (1.0 + ez)
            r = (sig - t) * (1.0 / rows)
            rrow = jnp.concatenate([r[q:q + 1, :] for q in range(q_n)], axis=1)
            rscaled = rrow * (out_scale * in_scale)
            for g in range(hid // 16):
                sl = slice(16 * g, 16 * g + 16)
                h = act[sl, cols]
                w2t = jnp.concatenate([w2b[sl, :]] * q_n, axis=1)
                hr = h * rrow
                s = hr[:, :LANES]
                for q in range(1, q_n):
                    s = s + hr[:, LANES * q:LANES * (q + 1)]
                gcol[g] = gcol[g] + s
                d = rscaled * w2t * (1.0 - h * h)
                for ref, val in zip((d_hi, d_mid, d_lo), split3(d)):
                    ref[c % 2, sl, :] = val
            prod = exact_dot([ref[c % 2] for ref in (d_hi, d_mid, d_lo)], x_ref[cols, :], NN)
            if c == 0:
                hist_y[n0, :, :dim] = prod
            else:
                hist_y[n0, :, :dim] = hist_y[n0, :, :dim] + prod
        loss_ref[k] = jnp.sum(loss_acc) * (1.0 / rows)
        for g in range(hid // 16):
            sl = slice(16 * g, 16 * g + 16)
            hist_y[n0, sl, dim:dim + 1] = jnp.sum(gcol[g], axis=1, keepdims=True) * out_scale

        def dots(i, accs):
            base = pl.multiple_of(i * 16, 16)
            sl = pl.ds(base, 16)
            accs = list(accs)
            for b in range(wide // LANES):
                ln = slice(LANES * b, LANES * (b + 1))
                gk = hist_y[n0, sl, ln] + lam * theta[sl, ln]
                y0 = jnp.where(live, gk - grad[sl, ln], 0.0)
                grad[sl, ln] = gk
                hist_y[n0, sl, ln] = y0
                s0 = hist_s[n0, sl, ln]
                s1 = hist_s[n1, sl, ln]
                s2 = hist_s[n2, sl, ln]
                y1 = hist_y[n1, sl, ln]
                y2 = hist_y[n2, sl, ln]
                for n, (u, v) in enumerate(((s0, gk), (y0, gk), (y0, y0), (y0, y1), (y0, y2), (s0, y0), (s1, y0), (s2, y0))):
                    accs[n] = accs[n] + u * v
            return tuple(accs)

        accs = lax.fori_loop(0, hid // 16, dots, tuple(jnp.zeros((16, LANES), F32) for _ in range(8)))
        for n in range(8):
            dbuf[me, n:n + 1, :] = sub_sum(accs[n])
        for off in range(1, feat):
            d_copy(off).start()
        for off in range(1, feat):
            d_copy(off).wait()
        tot = dbuf[0]
        for src in range(1, feat):
            tot = tot + dbuf[src]
        tot = jnp.broadcast_to(jnp.sum(tot, axis=1, keepdims=True), (8, LANES))
        sg0, yg0, yy00, yy01, yy02, sy00, sy01, sy02 = [jnp.broadcast_to(tot[n:n + 1, :], (8, LANES)) for n in range(8)]
        sg1 = sg0p + sy01
        sg2 = sg1p + sy02
        yg1 = yg0p + yy01
        yg2 = yg1p + yy02
        yy11, yy12, yy22 = yy00p, yy01p, yy11p
        sy12 = sy01p
        rho0 = jnp.where(live, 1.0 / sy00, 0.0)
        gamma = jnp.where(live, sy00 / yy00, 1.0)
        rho1, rho2 = rho0p, rho1p
        a0 = rho0 * sg0
        a1 = rho1 * (sg1 - a0 * sy01)
        a2 = rho2 * (sg2 - a0 * sy02 - a1 * sy12)
        b2 = rho2 * gamma * (yg2 - a0 * yy02 - a1 * yy12 - a2 * yy22)
        e2 = a2 - b2
        b1 = rho1 * (gamma * (yg1 - a0 * yy01 - a1 * yy11 - a2 * yy12) + e2 * sy12)
        e1 = a1 - b1
        b0 = rho0 * (gamma * (yg0 - a0 * yy00 - a1 * yy01 - a2 * yy02) + e2 * sy02 + e1 * sy01)
        e0 = a0 - b0
        coefs = [-alpha * gamma, alpha * gamma * a0, alpha * gamma * a1, alpha * gamma * a2, -alpha * e0, -alpha * e1, -alpha * e2]
        coefs = [jnp.concatenate([v, v], axis=0) for v in coefs]

        def update(i, none):
            base = pl.multiple_of(i * 16, 16)
            sl = pl.ds(base, 16)
            for b in range(wide // LANES):
                ln = slice(LANES * b, LANES * (b + 1))
                old = theta[sl, ln]
                step = coefs[0] * grad[sl, ln]
                for n, (ref, slot) in enumerate(((hist_y, n0), (hist_y, n1), (hist_y, n2), (hist_s, n0), (hist_s, n1), (hist_s, n2))):
                    step = step + coefs[n + 1] * ref[slot, sl, ln]
                new = old + step
                theta[sl, ln] = new
                hist_s[n2, sl, ln] = new - old
                for ref, val in zip(parts_refs, split3(new)):
                    ref[sl, ln] = val
            return none

        lax.fori_loop(0, hid // 16, update, 0)
        w2b[...] = jnp.broadcast_to(theta[:, dim:dim + 1], (hid, LANES))
        return rho0, rho1, sg0, sg1, yg0, yg1, yy00, yy01, yy11, sy01

    lax.fori_loop(0, NUM_ITERS, iteration, tuple(row1 for _ in range(10)))
    wout_ref[...] = theta[:, :dim]
    for j in range(hid // LANES):
        w2out_ref[j:j + 1, :] = jnp.transpose(w2b[j * LANES:(j + 1) * LANES, :])[0:1, :]


def solution(mesh):
    feat = mesh.shape["feat"]

    def local_solve(x_loc, t_loc, win_loc, wout_loc, reg_loc, step_loc):
        rows, dim = x_loc.shape
        hid = win_loc.shape[0]
        wide = (dim // LANES + 1) * LANES
        n_chunks = rows // CHUNK
        q_n = CHUNK // LANES
        vmem = pl.BlockSpec(memory_space=pltpu.VMEM)
        smem = pl.BlockSpec(memory_space=pltpu.SMEM)
        w_new, w2_new, losses = pl.pallas_call(
            functools.partial(kernel, feat),
            out_shape=(jax.ShapeDtypeStruct((hid, dim), F32), jax.ShapeDtypeStruct((hid // LANES, LANES), F32),
                       jax.ShapeDtypeStruct((NUM_ITERS,), F32)),
            in_specs=[smem, smem, vmem, vmem, vmem, vmem],
            out_specs=(vmem, vmem, smem),
            scratch_shapes=[
                pltpu.VMEM((hid, wide), F32), pltpu.VMEM((hid, wide), F32),
                pltpu.VMEM((HIST, hid, wide), F32), pltpu.VMEM((HIST, hid, wide), F32),
                pltpu.VMEM((hid, wide), BF16), pltpu.VMEM((hid, wide), BF16), pltpu.VMEM((hid, wide), BF16),
                pltpu.VMEM((hid, rows), F32), pltpu.VMEM((hid, LANES), F32),
                pltpu.VMEM((2, hid, CHUNK), BF16), pltpu.VMEM((2, hid, CHUNK), BF16), pltpu.VMEM((2, hid, CHUNK), BF16),
                pltpu.VMEM((feat, n_chunks, q_n, LANES), F32), pltpu.VMEM((feat, 8, LANES), F32),
                pltpu.SemaphoreType.DMA((n_chunks, feat - 1)), pltpu.SemaphoreType.DMA((n_chunks, feat - 1)),
                pltpu.SemaphoreType.DMA((feat - 1,)), pltpu.SemaphoreType.DMA((feat - 1,)),
            ],
            compiler_params=pltpu.CompilerParams(collective_id=0, has_side_effects=True),
        )(reg_loc, step_loc, x_loc, t_loc.reshape(n_chunks, q_n, LANES), win_loc, wout_loc.reshape(hid // LANES, LANES))
        return w_new, w2_new.reshape(hid), losses

    specs_in = (P("prob", None), P("prob"), P(("prob", "feat"), None), P(("prob", "feat")), P("prob"), P("prob"))
    specs_out = (P(("prob", "feat"), None), P(("prob", "feat")), P("prob"))
    return jax.shard_map(local_solve, mesh=mesh, in_specs=specs_in, out_specs=specs_out, check_vma=False)
```

```python
import functools
import math

import jax
import jax.numpy as jnp
from jax import lax
from jax.experimental import pallas as pl
from jax.experimental.pallas import tpu as pltpu
from jax.sharding import PartitionSpec as P

NUM_ITERS = 6
HIST = 3
LANES = 128
CHUNK = 512
F32 = jnp.float32
BF16 = jnp.bfloat16
NT = (((1,), (1,)), ((), ()))
NN = (((1,), (0,)), ((), ()))


def split3(val):
    hi = val.astype(BF16)
    rest = val - hi.astype(F32)
    mid = rest.astype(BF16)
    lo = (rest - mid.astype(F32)).astype(BF16)
    return hi, mid, lo


def exact_dot(parts, rhs, dims):
    out = lax.dot_general(parts[0], rhs, dims, preferred_element_type=F32)
    for part in parts[1:]:
        out = out + lax.dot_general(part, rhs, dims, preferred_element_type=F32)
    return out


def sub_sum(val):
    return jnp.sum(val, axis=0, keepdims=True)


def spread(col):
    return jnp.broadcast_to(col, (col.shape[0], LANES))


def kernel(feat, reg_ref, step_ref, x_hbm, t_ref, w_ref, w2_ref, wout_ref, w2out_ref, loss_ref,
           x_ref, x_tail, theta, grad, gacc, hist_s, hist_y, p_hi, p_mid, p_lo, p_tail, pbase, ubuf, act, w2base, gw, w2b,
           d_hi, d_mid, d_lo, kept, zbuf, dbuf, x_sem, z_send, z_recv, d_send, d_recv):
    dim, rows = x_ref.shape
    hid = w_ref.shape[1]
    tall = theta.shape[0]
    main = dim // LANES * LANES
    tail = dim - main
    n_chunks = rows // CHUNK
    q_n = CHUNK // LANES
    in_scale = 1.0 / math.sqrt(dim)
    out_scale = 1.0 / math.sqrt(hid * feat)
    me = lax.axis_index("feat")
    parts_refs = (p_hi, p_mid, p_lo)
    cols_of = [slice(CHUNK * c, CHUNK * (c + 1)) for c in range(n_chunks)]

    def x_copy(c):
        return pltpu.make_async_copy(x_hbm.at[:, cols_of[c]], x_ref.at[:, cols_of[c]], x_sem.at[c])

    for c in range(n_chunks):
        x_copy(c).start()
    barrier = pltpu.get_barrier_semaphore()
    for off in range(1, feat):
        pl.semaphore_signal(barrier, inc=1, device_id={"feat": lax.rem(me + off, feat)}, device_id_type=pl.DeviceIdType.MESH)

    def z_copy(c, off):
        return pltpu.make_async_remote_copy(
            src_ref=zbuf.at[me, c], dst_ref=zbuf.at[me, c], send_sem=z_send.at[c, off - 1], recv_sem=z_recv.at[c, off - 1],
            device_id={"feat": lax.rem(me + off, feat)}, device_id_type=pl.DeviceIdType.MESH)

    def d_copy(off):
        return pltpu.make_async_remote_copy(
            src_ref=dbuf.at[me], dst_ref=dbuf.at[me], send_sem=d_send.at[off - 1], recv_sem=d_recv.at[off - 1],
            device_id={"feat": lax.rem(me + off, feat)}, device_id_type=pl.DeviceIdType.MESH)

    lam = jnp.broadcast_to(reg_ref[...], (8, hid))
    alpha = jnp.broadcast_to(step_ref[...], (8, LANES))
    lane = lax.broadcasted_iota(jnp.int32, (LANES, LANES), 1)
    lane8 = lax.broadcasted_iota(jnp.int32, (8, LANES), 1)

    def store_parts(ref):
        for b in range(main // LANES):
            ln = slice(LANES * b, LANES * (b + 1))
            for j in range(hid // LANES):
                sl = slice(LANES * j, LANES * (j + 1))
                for part, val in zip(parts_refs, split3(jnp.transpose(ref[ln, sl]))):
                    part[sl, ln] = val
        for j in range(hid // LANES):
            sl = slice(LANES * j, LANES * (j + 1))
            block = jnp.concatenate([ref[main:dim, sl], jnp.zeros((LANES - tail, LANES), F32)], axis=0)
            hi, mid, lo = [v.astype(F32) for v in split3(jnp.transpose(block))]
            both = jnp.where(lane < tail, hi, jnp.where(lane < 2 * tail, pltpu.roll(mid, tail, 1), pltpu.roll(lo, 2 * tail, 1)))
            p_tail[sl, :] = both.astype(BF16)

    def image(c):
        out = exact_dot([ref[...] for ref in parts_refs], x_ref[:main, cols_of[c]], NN)
        return out + lax.dot_general(p_tail[:, :3 * tail], x_tail[:, cols_of[c]], NN, preferred_element_type=F32)

    def activate(c, pre_of):
        cols = cols_of[c]
        acc = jnp.zeros((8, CHUNK), F32)
        for g in range(hid // 8):
            sl = slice(8 * g, 8 * g + 8)
            h = jnp.tanh(pre_of(sl, cols))
            act[sl, cols] = h
            acc = acc + h * jnp.concatenate([w2b[sl, :]] * q_n, axis=1)
        zrow = sub_sum(acc) * out_scale
        for q in range(q_n):
            zbuf[me, c, q:q + 1, :] = zrow[:, LANES * q:LANES * (q + 1)]
        for off in range(1, feat):
            z_copy(c, off).start()

    def new_theta(n0, n1, n2, coefs, sl):
        old = theta[sl, :]
        step = coefs[0] * grad[sl, :]
        for n, (ref, slot) in enumerate(((hist_y, n0), (hist_y, n1), (hist_y, n2), (hist_s, n0), (hist_s, n1), (hist_s, n2))):
            step = step + coefs[n + 1] * ref[slot, sl, :]
        return old, old + step

    def widen(coefs):
        return [jnp.concatenate([v] * (hid // LANES), axis=1) for v in coefs]

    def backward(k, n0, n1, n2, live):
        loss_acc = [jnp.zeros((q_n, LANES), F32)]
        gcol = [jnp.zeros((16, LANES), F32) for _ in range(hid // 16)]
        accs = [jnp.zeros((8, hid), F32) for _ in range(8)]
        moves = widen([kept[16 + n] for n in range(7)])

        def update(lo, hi):
            for g in range(lo // 8, hi // 8):
                sl = slice(8 * g, 8 * g + 8)
                old, new = new_theta(n1, n2, n0, moves, sl)
                theta[sl, :] = new
                hist_s[n0, sl, :] = new - old

        def finish(lo, hi, fresh):
            for g in range(lo // 8, hi // 8):
                sl = slice(8 * g, 8 * g + 8)
                plain = gacc[sl, :]
                if fresh is not None:
                    plain = plain + fresh[8 * g - lo:8 * g - lo + 8, :]
                gk = plain + lam * theta[sl, :]
                y0 = jnp.where(live, gk - grad[sl, :], 0.0)
                grad[sl, :] = gk
                hist_y[n0, sl, :] = y0
                s0 = hist_s[n0, sl, :]
                s1 = hist_s[n1, sl, :]
                s2 = hist_s[n2, sl, :]
                y1 = hist_y[n1, sl, :]
                y2 = hist_y[n2, sl, :]
                for n, (u, v) in enumerate(((s0, gk), (y0, gk), (y0, y0), (y0, y1), (y0, y2), (s0, y0), (s1, y0), (s2, y0))):
                    accs[n] = accs[n] + u * v

        def arrive(c):
            for off in range(1, feat):
                z_copy(c, off).wait()

        def slope(c):
            cols = cols_of[c]
            z = zbuf[0, c]
            for src in range(1, feat):
                z = z + zbuf[src, c]
            t = t_ref[c]
            ez = jnp.exp(-jnp.abs(z))
            loss_acc[0] = loss_acc[0] + (jnp.maximum(z, 0.0) + jnp.log1p(ez) - t * z)
            sig = jnp.where(z >= 0.0, 1.0, ez) / (1.0 + ez)
            r = (sig - t) * (1.0 / rows)
            rrow = jnp.concatenate([r[q:q + 1, :] for q in range(q_n)], axis=1)
            rscaled = rrow * (out_scale * in_scale)
            for g in range(hid // 16):
                sl = slice(16 * g, 16 * g + 16)
                h = act[sl, cols]
                w2t = jnp.concatenate([w2b[sl, :]] * q_n, axis=1)
                hr = h * rrow
                s = hr[:, :LANES]
                for q in range(1, q_n):
                    s = s + hr[:, LANES * q:LANES * (q + 1)]
                gcol[g] = gcol[g] + s
                d = rscaled * w2t * (1.0 - h * h)
                for ref, val in zip((d_hi, d_mid, d_lo), split3(d)):
                    ref[c, sl, :] = val

        def product(c, lo, hi):
            lhs = x_ref[lo:hi, cols_of[c]]
            out = lax.dot_general(lhs, d_hi[c], NT, preferred_element_type=F32)
            out = out + lax.dot_general(lhs, d_mid[c], NT, preferred_element_type=F32)
            return out + lax.dot_general(lhs, d_lo[c], NT, preferred_element_type=F32)

        half = dim // 32 * 16
        arrive(0)
        slope(0)
        arrive(1)
        gacc[:dim, :] = product(0, 0, dim)
        slope(1)
        update(0, half)
        arrive(2)
        gacc[:dim, :] = gacc[:dim, :] + product(1, 0, dim)
        slope(2)
        update(half, tall)
        arrive(3)
        gacc[:dim, :] = gacc[:dim, :] + product(2, 0, dim)
        slope(3)
        cols = []
        for j in range(hid // LANES):
            block = jnp.concatenate(gcol[j * (LANES // 16):(j + 1) * (LANES // 16)], axis=0)
            gacc[dim:dim + 1, LANES * j:LANES * (j + 1)] = sub_sum(jnp.transpose(block)) * out_scale
            cols.append(jnp.sum(block, axis=1, keepdims=True) * out_scale)
        first = dim - 2 * 256
        edges = (0, first, first + 256, dim)
        for lo, hi in zip(edges[:-1], edges[1:]):
            finish(lo, hi, product(3, lo, hi))
            if lo == 0:
                finish(dim, tall, None)
        for n in range(8):
            total = accs[n][:, :LANES]
            for j in range(1, hid // LANES):
                total = total + accs[n][:, LANES * j:LANES * (j + 1)]
            dbuf[me, n:n + 1, :] = sub_sum(total)
        for off in range(1, feat):
            d_copy(off).start()
        loss_ref[k] = jnp.sum(loss_acc[0]) * (1.0 / rows)
        return cols

    def direction(live, carry):
        rho0p, rho1p, sg0p, sg1p, yg0p, yg1p, yy00p, yy01p, yy11p, sy01p = carry
        for off in range(1, feat):
            d_copy(off).wait()
        tot = dbuf[0]
        for src in range(1, feat):
            tot = tot + dbuf[src]
        tot = spread(jnp.sum(tot, axis=1, keepdims=True))
        sg0, yg0, yy00, yy01, yy02, sy00, sy01, sy02 = [jnp.broadcast_to(tot[n:n + 1, :], (8, LANES)) for n in range(8)]
        sg1 = sg0p + sy01
        sg2 = sg1p + sy02
        yg1 = yg0p + yy01
        yg2 = yg1p + yy02
        yy11, yy12, yy22 = yy00p, yy01p, yy11p
        sy12 = sy01p
        rho0 = jnp.where(live, 1.0 / sy00, 0.0)
        gamma = jnp.where(live, sy00 / yy00, 1.0)
        rho1, rho2 = rho0p, rho1p
        a0 = rho0 * sg0
        a1 = rho1 * (sg1 - a0 * sy01)
        a2 = rho2 * (sg2 - a0 * sy02 - a1 * sy12)
        b2 = rho2 * gamma * (yg2 - a0 * yy02 - a1 * yy12 - a2 * yy22)
        e2 = a2 - b2
        b1 = rho1 * (gamma * (yg1 - a0 * yy01 - a1 * yy11 - a2 * yy12) + e2 * sy12)
        e1 = a1 - b1
        b0 = rho0 * (gamma * (yg0 - a0 * yy00 - a1 * yy01 - a2 * yy02) + e2 * sy02 + e1 * sy01)
        e0 = a0 - b0
        neg = -alpha
        ng = neg * gamma
        coefs = [ng, -ng * a0, -ng * a1, -ng * a2, neg * e0, neg * e1, neg * e2]
        return coefs, (rho0, rho1, sg0, sg1, yg0, yg1, yy00, yy01, yy11, sy01)

    for j in range(hid // LANES):
        w2base[j * LANES:(j + 1) * LANES, :] = jnp.transpose(jnp.broadcast_to(w2_ref[j:j + 1, :], (LANES, LANES)))
    theta[:dim, :] = w_ref[...]
    w2_row = jnp.concatenate([w2_ref[j:j + 1, :] for j in range(hid // LANES)], axis=1)
    below = lax.broadcasted_iota(jnp.int32, (tall - dim, hid), 0)
    theta[dim:, :] = jnp.where(below == 0, jnp.broadcast_to(w2_row, (tall - dim, hid)), 0.0)
    w2b[...] = w2base[...]
    store_parts(theta)
    for ref in (hist_s, hist_y, grad, ubuf, gw, kept):
        ref[...] = jnp.zeros_like(ref)
    gacc[dim:, :] = jnp.zeros((tall - dim, hid), F32)
    pl.semaphore_wait(barrier, feat - 1)

    for c in range(n_chunks + 1):
        if c < n_chunks:
            cols = cols_of[c]
            x_copy(c).wait()
            for n in range(3):
                x_tail[tail * n:tail * (n + 1), cols] = x_ref[main:, cols]
            pbase[:, cols] = image(c) * in_scale
        if c > 0:
            activate(c - 1, lambda sl, ln: pbase[sl, ln])

    def iteration(k, none):
        carry = [kept[n] for n in range(10)]
        s0, s1, s2, y1, y2, total = [kept[n] for n in range(10, 16)]
        n0 = lax.rem(k, HIST)
        n1 = lax.rem(k + 2, HIST)
        n2 = lax.rem(k + 1, HIST)
        live = k > 0
        cols = backward(k, n0, n1, n2, live)
        store_parts(grad)
        lam_col = lam[:, :LANES]
        for j, col in enumerate(cols):
            for g in range(LANES // 8):
                sl = slice(LANES * j + 8 * g, LANES * j + 8 * g + 8)
                gw[k, sl, :] = spread(col[8 * g:8 * g + 8, :]) + lam_col * w2b[sl, :]
        for c in range(n_chunks - 1):
            ubuf[k, :, cols_of[c]] = image(c) * in_scale
        coefs, carry = direction(live, carry)
        here = jnp.where(lane8 == k, 1.0, 0.0)
        y_new = jnp.where(live, here - jnp.where(lane8 == k - 1, 1.0, 0.0), 0.0)
        move = coefs[0] * here
        for coef, vec in zip(coefs[1:], (y_new, y1, y2, s0, s1, s2)):
            move = move + coef * vec
        total = total + move
        e = [spread(total[:, j:j + 1]) for j in range(NUM_ITERS - 1)]
        for g in range(hid // 8):
            sl = slice(8 * g, 8 * g + 8)
            val = w2base[sl, :]
            for j in range(NUM_ITERS - 1):
                val = val + e[j] * gw[j, sl, :]
            w2b[sl, :] = val
        e_wide = [jnp.concatenate([v] * q_n, axis=1) for v in e]

        def pre_of(sl, cols):
            val = pbase[sl, cols]
            for j in range(NUM_ITERS - 1):
                val = val + e_wide[j] * ubuf[j, sl, cols]
            return val

        for c in range(n_chunks):
            if c == n_chunks - 2:
                ubuf[k, :, cols_of[c + 1]] = image(c + 1) * in_scale
            activate(c, pre_of)
        for n, val in enumerate((*carry, move, s0, s1, y_new, y1, total, *coefs)):
            kept[n] = val
        return none

    lax.fori_loop(0, NUM_ITERS - 1, iteration, 0)

    last = NUM_ITERS - 1
    n0, n1, n2 = last % HIST, (last + 2) % HIST, (last + 1) % HIST
    backward(last, n0, n1, n2, True)
    coefs, _ = direction(True, [kept[n] for n in range(10)])
    coefs = widen(coefs)
    for g in range(dim // 8):
        sl = slice(8 * g, 8 * g + 8)
        wout_ref[sl, :] = new_theta(n0, n1, n2, coefs, sl)[1]
    row = new_theta(n0, n1, n2, coefs, slice(dim, dim + 8))[1][0:1, :]
    for j in range(hid // LANES):
        w2out_ref[j:j + 1, :] = row[:, LANES * j:LANES * (j + 1)]


def hand_on(w_ref, w2_ref, loss_ref, w_out, w2_out, loss_out):
    w_out[...] = w_ref[...]
    w2_out[...] = w2_ref[...]
    for k in range(NUM_ITERS):
        loss_out[k] = loss_ref[k]


def solution(mesh):
    feat = mesh.shape["feat"]

    def local_solve(x_loc, t_loc, win_loc, wout_loc, reg_loc, step_loc):
        rows, dim = x_loc.shape
        hid = win_loc.shape[0]
        tall = dim + 8
        main = dim // LANES * LANES
        n_chunks = rows // CHUNK
        q_n = CHUNK // LANES
        vmem = pl.BlockSpec(memory_space=pltpu.VMEM)
        smem = pl.BlockSpec(memory_space=pltpu.SMEM)
        w_new, w2_new, losses = pl.pallas_call(
            functools.partial(kernel, feat),
            out_shape=(jax.ShapeDtypeStruct((dim, hid), F32), jax.ShapeDtypeStruct((hid // LANES, LANES), F32),
                       jax.ShapeDtypeStruct((NUM_ITERS,), F32)),
            in_specs=[vmem, vmem, pl.BlockSpec(memory_space=pl.ANY), vmem, vmem, vmem],
            out_specs=(vmem, vmem, smem),
            scratch_shapes=[
                pltpu.VMEM((dim, rows), BF16), pltpu.VMEM((3 * (dim - main), rows), BF16),
                pltpu.VMEM((tall, hid), F32), pltpu.VMEM((tall, hid), F32), pltpu.VMEM((tall, hid), F32),
                pltpu.VMEM((HIST, tall, hid), F32), pltpu.VMEM((HIST, tall, hid), F32),
                pltpu.VMEM((hid, main), BF16), pltpu.VMEM((hid, main), BF16), pltpu.VMEM((hid, main), BF16),
                pltpu.VMEM((hid, LANES), BF16),
                pltpu.VMEM((hid, rows), F32), pltpu.VMEM((NUM_ITERS - 1, hid, rows), F32), pltpu.VMEM((hid, rows), F32),
                pltpu.VMEM((hid, LANES), F32), pltpu.VMEM((NUM_ITERS - 1, hid, LANES), F32), pltpu.VMEM((hid, LANES), F32),
                pltpu.VMEM((4, hid, CHUNK), BF16), pltpu.VMEM((4, hid, CHUNK), BF16), pltpu.VMEM((4, hid, CHUNK), BF16),
                pltpu.VMEM((23, 8, LANES), F32),
                pltpu.VMEM((feat, n_chunks, q_n, LANES), F32), pltpu.VMEM((feat, 8, LANES), F32),
                pltpu.SemaphoreType.DMA((n_chunks,)),
                pltpu.SemaphoreType.DMA((n_chunks, feat - 1)), pltpu.SemaphoreType.DMA((n_chunks, feat - 1)),
                pltpu.SemaphoreType.DMA((feat - 1,)), pltpu.SemaphoreType.DMA((feat - 1,)),
            ],
            compiler_params=pltpu.CompilerParams(collective_id=0, has_side_effects=True),
        )(reg_loc.reshape(1, 1), step_loc.reshape(1, 1), x_loc.T, t_loc.reshape(n_chunks, q_n, LANES), win_loc.T, wout_loc.reshape(hid // LANES, LANES))
        w_new, w2_new, losses = pl.pallas_call(
            hand_on,
            out_shape=(jax.ShapeDtypeStruct((dim, hid), F32), jax.ShapeDtypeStruct((hid // LANES, LANES), F32),
                       jax.ShapeDtypeStruct((NUM_ITERS,), F32)),
            in_specs=[vmem, vmem, smem],
            out_specs=(vmem, vmem, smem),
        )(w_new, w2_new, losses)
        return w_new.T, w2_new.reshape(hid), losses

    specs_in = (P("prob", None), P("prob"), P(("prob", "feat"), None), P(("prob", "feat")), P("prob"), P("prob"))
    specs_out = (P(("prob", "feat"), None), P(("prob", "feat")), P("prob"))
    return jax.shard_map(local_solve, mesh=mesh, in_specs=specs_in, out_specs=specs_out, check_vma=False)
```
